32 devices in a mesh: dp: 4 (over z), tensor: 8 (over y, x, core).
Axes of the slice: x: 2, y: 2, z: 4, core: 2. Of those that a mesh axis runs over, the one named last changes fastest.
Arguments:
- tokens: bfloat16 [4, 1024, 4096], P('dp', 'tensor'), may hold values from -1.8 to 1.8
- cotangent: bfloat16 [4, 1024, 4096], P('dp', None, 'tensor'), may hold values from -6 to 6
- gain: float32 [4096], replicated, may hold values from 0.25 to 3.5
- w_query: bfloat16 [4096, 4096], P(None, 'tensor'), may hold values from -6 to 6
- w_key: bfloat16 [4096, 512], P(None, 'tensor'), may hold values from -6 to 6
- w_value: bfloat16 [4096, 512], P(None, 'tensor'), may hold values from -6 to 6
- moment_query: float32 [4096, 4096], P('dp', 'tensor'), may hold values from -6 to 6
- moment_key: float32 [4096, 512], P('dp', 'tensor'), may hold values from -6 to 6
- moment_value: float32 [4096, 512], P('dp', 'tensor'), may hold values from -6 to 6
Outputs:
- attended: bfloat16 [4, 1024, 4096], P('dp', None, 'tensor')
- grad_tokens: bfloat16 [4, 1024, 4096], P('dp', 'tensor')
- fresh_query: bfloat16 [4096, 4096], P(None, 'tensor')
- fresh_key: bfloat16 [4096, 512], P(None, 'tensor')
- fresh_value: bfloat16 [4096, 512], P(None, 'tensor')
- next_query: float32 [4096, 4096], P('dp', 'tensor')
- next_key: float32 [4096, 512], P('dp', 'tensor')
- next_value: float32 [4096, 512], P('dp', 'tensor')
The draws below stay inside these ranges and needn't reach their ends.
All inputs are finite; a program needn't handle non-finite values.
Results may differ from the reference program's by a relative error of at most 0.017.
Values may be sent and summed in bfloat16 or wider, within the bound.
No kernel may reach another device: no remote copies, remote signals or barrier semaphores. Data moves between devices by JAX's collectives and lax.ppermute only.
A program may use at most 256 MiB of HBM per device.

```python
import jax
import jax.numpy as jnp
from jax import lax

D = 4096
HEADS = 32
KVH = 4
HD = 128
SEQ = 1024
SEQS = 4
N_TENSOR = 8


def drawn_weight(key, columns, salt):
    base = jnp.clip(jax.random.normal(jax.random.fold_in(key, salt), (D, columns), jnp.float32), -6.0, 6.0)
    return base


def draw_tokens(key, part):
    noise = jax.random.normal(jax.random.fold_in(key, 21), (SEQS, SEQ, D), jnp.float32)
    values = 0.3 * noise
    return jnp.clip(values, -1.8, 1.8).astype(jnp.bfloat16)


def draw_gain(key, part):
    spot = jnp.arange(D, dtype=jnp.float32) / (D - 1.0)
    rough = jax.random.uniform(jax.random.fold_in(key, 31), (D,), jnp.float32, 0.85, 1.15)
    trend = 0.5 + spot
    return trend * rough


def draw_w_query(key, part):
    return drawn_weight(key, HEADS * HD, 11).astype(jnp.bfloat16)


def draw_w_key(key, part):
    return drawn_weight(key, KVH * HD, 12).astype(jnp.bfloat16)


def block_levels(own_key, dims, shards, low, high):
    level = 1.0
    for position, parts in shards:
        steps = jax.random.uniform(jax.random.fold_in(jax.random.fold_in(own_key, 6), position), (parts,), jnp.float32, low / len(shards), high / len(shards))
        level = level * jnp.repeat(jnp.exp(steps), dims[position] // parts).reshape((-1,) + (1,) * (len(dims) - 1 - position))
    return level


def centred(rng, dims, scale, most, cuts=(), kind=jnp.bfloat16):
    result = scale * jax.random.normal(rng, dims, jnp.float32)
    if cuts:
        result = result * block_levels(rng, dims, cuts, -0.22, 0.18)
    return jnp.clip(result, -most, most).astype(kind)


def setup_inputs(seed: int = 0) -> dict:
    seeds = jax.random.split(jax.random.key(seed), 10)
    return {
        "tokens": draw_tokens(jax.random.fold_in(seeds[9], 71), 0),
        "cotangent": centred(seeds[1], (SEQS, SEQ, HEADS * HD), 1.0, 6.0, ((0, 4), (2, 8))),
        "gain": draw_gain(jax.random.fold_in(seeds[9], 71), 0),
        "w_query": draw_w_query(jax.random.fold_in(seeds[9], 71), 0),
        "w_key": draw_w_key(jax.random.fold_in(seeds[9], 71), 0),
        "w_value": centred(seeds[5], (D, KVH * HD), 1.0, 6.0, ((1, 8),)),
        "moment_query": centred(seeds[6], (D, HEADS * HD), 1.0, 6.0, ((0, 4), (1, 8)), jnp.float32),
        "moment_key": centred(seeds[7], (D, KVH * HD), 1.0, 6.0, ((0, 4), (1, 8)), jnp.float32),
        "moment_value": centred(seeds[8], (D, KVH * HD), 1.0, 6.0, ((0, 4), (1, 8)), jnp.float32),
    }


rope_base = 1000000.0
norm_eps = 1e-06
stat_eps = 1e-06
learn_rate = 0.05
keep_rate = 0.9

def rotate(matrix, first_column, head_size, sign):
    length = matrix.shape[0]
    columns = matrix.shape[1]
    index = first_column + jnp.arange(columns, dtype=jnp.int32)
    within = index % head_size // 2
    rates = jnp.power(jnp.float32(rope_base), within.astype(jnp.float32) * (-2.0 / head_size))
    angle = jnp.arange(length, dtype=jnp.float32)[:, None] * rates[None, :]
    even = index % 2 == 0
    partner = jnp.where(even[None, :], -jnp.roll(matrix, -1, axis=1), jnp.roll(matrix, 1, axis=1))
    return matrix * jnp.cos(angle) + partner * (sign * jnp.sin(angle))

def settle(values):
    return lax.optimization_barrier(values.astype(jnp.bfloat16)).astype(jnp.float32)

def split_columns(matrix, count):
    return matrix.reshape(matrix.shape[0], N_TENSOR, count).transpose(1, 0, 2)

def sequence_pass(tokens_one, grad_one, gain, w_query, w_key, w_value):
    length = tokens_one.shape[0]
    width = tokens_one.shape[1]
    group = HEADS // KVH
    per_device = HEADS // N_TENSOR
    blocks = group // per_device
    in_scale = width ** (-0.5)
    head_scale = HD ** (-0.5)
    inputs = tokens_one.astype(jnp.float32)
    reciprocal = lax.rsqrt(lax.optimization_barrier(jnp.mean(inputs * inputs, axis=1, keepdims=True)) + norm_eps)
    unit_rows = inputs * reciprocal
    normed = (unit_rows * gain).astype(jnp.bfloat16)
    query = rotate(jnp.dot(normed, w_query, preferred_element_type=jnp.float32) * in_scale, 0, HD, 1.0).astype(jnp.bfloat16)
    keys = rotate(jnp.dot(normed, w_key, preferred_element_type=jnp.float32) * in_scale, 0, HD, 1.0).astype(jnp.bfloat16)
    values = (jnp.dot(normed, w_value, preferred_element_type=jnp.float32) * in_scale).astype(jnp.bfloat16)
    query_groups = query.reshape(length, KVH, group, HD).transpose(1, 2, 0, 3)
    grad_groups = grad_one.reshape(length, KVH, group, HD).transpose(1, 2, 0, 3)
    key_groups = keys.reshape(length, KVH, HD).transpose(1, 0, 2)
    value_groups = values.reshape(length, KVH, HD).transpose(1, 0, 2)
    places = jnp.arange(length)
    causal = places[:, None] >= places[None, :]

    def one_group(pieces):
        query_heads = pieces[0].astype(jnp.float32)
        grad_heads = pieces[1].astype(jnp.float32)
        key_head = pieces[2].astype(jnp.float32)
        value_head = pieces[3].astype(jnp.float32)
        scores = jnp.einsum('hsd,td->hst', query_heads, key_head) * head_scale
        attention = jax.nn.softmax(jnp.where(causal[None], scores, -1e+30), axis=2)
        attention_low = settle(attention)
        attended = jnp.einsum('hst,td->hsd', attention_low, value_head).astype(jnp.bfloat16)
        grad_raw = jnp.einsum('hsd,td->hst', grad_heads, value_head)
        grad_scores = attention * (grad_raw - lax.optimization_barrier(jnp.sum(attention * grad_raw, axis=2, keepdims=True)))
        grad_low = settle(grad_scores * head_scale)
        grad_query_raw = jnp.einsum('hst,td->hsd', grad_low, key_head)
        key_parts = jnp.einsum('hst,hsd->htd', grad_low, query_heads)
        value_parts = jnp.einsum('hst,hsd->htd', attention_low, grad_heads)
        key_sum = lax.optimization_barrier(jnp.sum(settle(key_parts.reshape(blocks, per_device, length, HD).sum(axis=1)), axis=0))
        value_sum = lax.optimization_barrier(jnp.sum(settle(value_parts.reshape(blocks, per_device, length, HD).sum(axis=1)), axis=0))
        return (attended, grad_query_raw, key_sum, value_sum)
    attended_g, query_g, key_g, value_g = lax.map(one_group, (query_groups, grad_groups, key_groups, value_groups))
    attended = attended_g.transpose(2, 0, 1, 3).reshape(length, HEADS * HD)
    grad_query_raw = query_g.transpose(2, 0, 1, 3).reshape(length, HEADS * HD)
    key_sums = key_g.transpose(1, 0, 2).reshape(length, KVH * HD)
    value_sums = value_g.transpose(1, 0, 2).reshape(length, KVH * HD)
    grad_key = rotate(key_sums, 0, HD, -1.0).astype(jnp.bfloat16)
    grad_value = value_sums.astype(jnp.bfloat16)
    grad_query = rotate(grad_query_raw, 0, HD, -1.0).astype(jnp.bfloat16)
    block = HEADS * HD // N_TENSOR
    key_block = KVH * HD // N_TENSOR

    def add_in(total, pieces):
        term = (jnp.dot(pieces[0], pieces[1].T, preferred_element_type=jnp.float32) + jnp.dot(pieces[2], pieces[3].T, preferred_element_type=jnp.float32) + jnp.dot(pieces[4], pieces[5].T, preferred_element_type=jnp.float32)) * in_scale
        return (total + settle(term), None)
    grad_normed, _ = lax.scan(add_in, jnp.zeros((length, width), jnp.float32), (split_columns(grad_query, block), split_columns(w_query, block), split_columns(grad_key, key_block), split_columns(w_key, key_block), split_columns(grad_value, key_block), split_columns(w_value, key_block)))
    grad_unit = grad_normed * gain
    inner = lax.optimization_barrier(jnp.mean(grad_unit * unit_rows, axis=1, keepdims=True))
    grad_tokens = (reciprocal * (grad_unit - unit_rows * inner)).astype(jnp.bfloat16)
    grad_wq = (jnp.dot(normed.T, grad_query, preferred_element_type=jnp.float32) * in_scale).astype(jnp.bfloat16)
    grad_wk = (jnp.dot(normed.T, grad_key, preferred_element_type=jnp.float32) * in_scale).astype(jnp.bfloat16)
    grad_wv = (jnp.dot(normed.T, grad_value, preferred_element_type=jnp.float32) * in_scale).astype(jnp.bfloat16)
    return (attended, grad_tokens, grad_wq, grad_wk, grad_wv)

def reference(tokens, cotangent, gain, w_query, w_key, w_value, moment_query, moment_key, moment_value):

    def single(pair):
        return sequence_pass(pair[0], pair[1], gain, w_query, w_key, w_value)
    attended, grad_tokens, stack_query, stack_key, stack_value = lax.map(single, (tokens, cotangent))
    sum_query = lax.optimization_barrier(jnp.sum(stack_query.astype(jnp.float32), axis=0))
    sum_key = lax.optimization_barrier(jnp.sum(stack_key.astype(jnp.float32), axis=0))
    sum_value = lax.optimization_barrier(jnp.sum(stack_value.astype(jnp.float32), axis=0))
    square = jnp.sum(sum_query * sum_query) + jnp.sum(sum_key * sum_key) + jnp.sum(sum_value * sum_value)
    count_all = 1.0 * D * HD * (HEADS + 2 * KVH)
    factor = lax.rsqrt(square / count_all + stat_eps)

    def advance(weight, moment, summed):
        moved = keep_rate * moment + summed * factor
        return ((weight.astype(jnp.float32) - learn_rate * moved).astype(jnp.bfloat16), moved)
    fresh_query, next_query = advance(w_query, moment_query, sum_query)
    fresh_key, next_key = advance(w_key, moment_key, sum_key)
    fresh_value, next_value = advance(w_value, moment_value, sum_value)
    return (attended, grad_tokens, fresh_query, fresh_key, fresh_value, next_query, next_key, next_value)
```

```python
import functools

import jax
import jax.numpy as jnp
from jax import lax
from jax.experimental import pallas as pl
from jax.experimental.pallas import tpu as pltpu
from jax.sharding import PartitionSpec as P


D = 4096
HEADS = 32
KVH = 4
HD = 128

rope_base = 1000000.0
norm_eps = 1e-06
stat_eps = 1e-06
learn_rate = 0.05
keep_rate = 0.9

BF = jnp.bfloat16
F32 = jnp.float32


def swap(shard, axis, mask):
    return lax.ppermute(shard, axis, [(i, i ^ mask) for i in range(lax.axis_size(axis))])


def after(value, *others):
    return lax.optimization_barrier((value,) + others)[0]


def slot_masks(size):
    return list(range(0, size, 2)) + list(range(1, size, 2))


def slot_of(mask, size):
    return mask // 2 + mask % 2 * (size // 2)


def gather_blocks(block, axis):
    size = lax.axis_size(axis)
    if size == 8:
        cut = block.shape[0] // 2
        top, low = block[:cut], block[cut:]
        y_top = swap(top, axis, 4)
        x_low = swap(low, axis, 2)
        y_low = swap(low, axis, 4)
        x_top = swap(top, axis, 2)
        far_top = swap(y_top, axis, 2)
        far_low = swap(x_low, axis, 4)
        even = {"t": top, "l": low, "xt": x_top, "xl": x_low, "yt": y_top, "yl": y_low}
        odd = [swap(piece, axis, 1) for piece in even.values()]
        far = [swap(far_top, axis, 1), swap(far_low, axis, 1)]
        return [(0, list(even.values()), odd), (3, [far_top, far_low], far)]
    even = [block]
    for level in range(1, size.bit_length() - 1):
        even = even + [swap(piece, axis, 1 << level) for piece in even]
    return [(0, even, [swap(piece, axis, 1) for piece in even])]


def scatter_blocks(even, odd, axis):
    size = lax.axis_size(axis)
    folded = (even.astype(F32) + swap(odd, axis, 1).astype(F32)).astype(BF)
    folded = folded.reshape(size // 2, -1, even.shape[1])
    if size == 8:
        cut = folded.shape[1] // 2
        top = swap(jnp.concatenate([folded[1, :cut], folded[3, :cut]], axis=0), axis, 2)
        bottom = swap(jnp.concatenate([folded[2, cut:], folded[3, cut:]], axis=0), axis, 4)
        top_y = (folded[2, :cut].astype(F32) + top[cut:].astype(F32)).astype(BF)
        bottom_x = (folded[1, cut:].astype(F32) + bottom[cut:].astype(F32)).astype(BF)
        top_y = swap(top_y, axis, 4)
        bottom_x = swap(bottom_x, axis, 2)
        own = folded[0].astype(F32)
        first = own[:cut] + top[:cut].astype(F32) + top_y.astype(F32)
        second = own[cut:] + bottom[:cut].astype(F32) + bottom_x.astype(F32)
        return jnp.concatenate([first, second], axis=0)
    held = {mask: folded[mask // 2].astype(F32) for mask in range(0, size, 2)}
    for level in range(1, size.bit_length() - 1):
        bit = 1 << level
        for mask in sorted(mask for mask in held if mask & bit):
            piece = held.pop(mask)
            held[mask ^ bit] = held[mask ^ bit] + swap(piece.astype(BF), axis, bit).astype(F32)
    return held[0]


def line_pairs(size, step, right):
    if right:
        return [(z, z + 1) for z in range(min(step, size - 1))]
    return [(z, z - 1) for z in range(max(size - step, 1), size)]


def line_scatter(terms, axis):
    size = lax.axis_size(axis)
    z = lax.axis_index(axis)
    rows = terms.shape[0] // size

    def own(index):
        return lax.dynamic_slice_in_dim(terms, index * rows, rows, 0)

    from_left = None
    from_right = None
    for step in range(1, size):
        if from_left is not None:
            terms, from_left, from_right = lax.optimization_barrier(
                (terms, from_left, from_right)
            )
        right = own((z + size - step) % size)
        left = own((z + step) % size)
        if from_left is not None:
            right = (right.astype(F32) + from_left.astype(F32)).astype(BF)
            left = (left.astype(F32) + from_right.astype(F32)).astype(BF)
        from_left = lax.ppermute(right, axis, line_pairs(size, step, True))
        from_right = lax.ppermute(left, axis, line_pairs(size, step, False))
    if size > 1:
        terms, from_left, from_right = lax.optimization_barrier((terms, from_left, from_right))
        return own(z).astype(F32) + from_left.astype(F32) + from_right.astype(F32)
    return own(z).astype(F32)


def line_gather(shard, axis):
    size = lax.axis_size(axis)
    z = lax.axis_index(axis)
    rows, columns = shard.shape
    rights = [shard]
    lefts = [shard]
    for step in range(1, size):
        pairs = [(i, i + 1) for i in range(step - 1, size - 1)]
        rights.append(lax.ppermute(rights[-1], axis, pairs))
        pairs = [(i, i - 1) for i in range(1, size - step + 1)]
        lefts.append(lax.ppermute(lefts[-1], axis, pairs))
    full = jnp.zeros((size * rows, columns), shard.dtype)
    full = lax.dynamic_update_slice(full, shard, (z * rows, 0))
    for k in range(1, size):
        piece = jnp.where(z >= k, rights[k], lefts[size - k])
        full = lax.dynamic_update_slice(full, piece, ((z - k) % size * rows, 0))
    return full


def sum_everywhere(value):
    for axis in ("tensor", "dp"):
        for level in range(lax.axis_size(axis).bit_length() - 1):
            value = value + swap(value, axis, 1 << level)
    return value[0, 0]


def rope_tables(rank, size, rows):
    blocks = rank ^ jnp.array(slot_masks(size), jnp.int32)
    places = (blocks[:, None] * rows + jnp.arange(rows, dtype=jnp.int32)[None, :]).reshape(-1)
    within = jnp.arange(HD, dtype=jnp.int32) // 2
    rates = jnp.power(F32(rope_base), within.astype(F32) * (-2.0 / HD))
    angle = places.astype(F32)[:, None] * rates[None, :]
    even = jnp.arange(HD, dtype=jnp.int32) % 2 == 0
    sin = jnp.sin(angle)
    return jnp.cos(angle), jnp.where(even[None, :], -sin, sin)


def turned(matrix, cos, sin):
    lane = lax.broadcasted_iota(jnp.int32, matrix.shape, 1)
    partner = jnp.where(
        lane % 2 == 0, pltpu.roll(matrix, HD - 1, 1), pltpu.roll(matrix, 1, 1)
    )
    return matrix * cos + partner * sin


def nt(a, b):
    return lax.dot_general(a, b, (((1,), (1,)), ((), ())), preferred_element_type=F32)


def nn(a, b):
    return lax.dot_general(a, b, (((1,), (0,)), ((), ())), preferred_element_type=F32)


def project_kernel(counts, *refs):
    even = refs[: counts[0]]
    odd = refs[counts[0] : counts[0] + counts[1]]
    w_query, w_pair = refs[counts[0] + counts[1] :][:2]
    out, rows_out = refs[-2:]
    query_width = w_query.shape[1]
    step = pl.program_id(0)

    @pl.when(step == 0)
    def _():
        out[...] = jnp.zeros_like(out)

    rows = jnp.concatenate([piece[...] for piece in even + odd], axis=0)
    rows_out[...] = rows.reshape(rows_out.shape)
    query = nn(rows, w_query[...])
    pair = nt(rows, w_pair[...])
    out[:, :, :query_width] += query.reshape(2, -1, query_width)
    out[:, :, query_width:] += pair.reshape(2, -1, w_pair.shape[0])


def project(first, even, odd, rows_each, size, w_query, w_pair, previous):
    width = w_query.shape[0]
    columns = w_query.shape[1] + w_pair.shape[0]
    half = size // 2 * rows_each
    rows = sum(piece.shape[0] for piece in even)
    chunk = min(width, 1024)
    pieces = list(even) + list(odd)
    operands = pieces + [w_query, w_pair]
    specs = [pl.BlockSpec((piece.shape[0], chunk), lambda k: (0, k)) for piece in pieces]
    specs.append(pl.BlockSpec((chunk, w_query.shape[1]), lambda k: (k, 0)))
    specs.append(pl.BlockSpec((w_pair.shape[0], chunk), lambda k: (0, k)))
    aliases = {}
    if previous is not None:
        aliases = {len(operands): 0, len(operands) + 1: 1}
        operands = operands + list(previous)
        specs = specs + [pl.BlockSpec(memory_space=pl.ANY)] * 2
    at = first * rows_each // rows
    return pl.pallas_call(
        functools.partial(project_kernel, (len(even), len(odd))),
        grid=(width // chunk,),
        in_specs=specs,
        out_specs=[
            pl.BlockSpec((2, rows, columns), lambda k: (0, at, 0)),
            pl.BlockSpec((2, rows, chunk), lambda k: (0, at, k)),
        ],
        out_shape=[
            jax.ShapeDtypeStruct((2, half, columns), F32),
            jax.ShapeDtypeStruct((2, half, width), BF),
        ],
        input_output_aliases=aliases,
        cost_estimate=pl.CostEstimate(
            flops=4 * rows * width * columns,
            transcendentals=0,
            bytes_accessed=8 * rows * width + 2 * width * columns,
        ),
        name="project",
    )(*operands)


def finish_kernel(factor_ref, w_ref, held_ref, full_ref, *rest):
    out = rest[-1]
    scaled = learn_rate * factor_ref[0, 0]
    out[...] = (
        w_ref[...].astype(F32) - held_ref[...].astype(F32) - scaled * full_ref[...].astype(F32)
    ).astype(BF)


def finish_query(factor, w_query, held, full, group, width, previous):
    rows = w_query.shape[0]
    block = min(rows, 1024)
    mine = lambda r: (r, group)
    operands = [factor, w_query, held, full]
    specs = [
        pl.BlockSpec(memory_space=pltpu.SMEM),
        pl.BlockSpec((block, width), mine),
        pl.BlockSpec((block, width), mine),
        pl.BlockSpec((block, width), lambda r: (r, 0)),
    ]
    aliases = {}
    if previous is not None:
        aliases = {4: 0}
        operands.append(previous)
        specs.append(pl.BlockSpec(memory_space=pl.ANY))
    return pl.pallas_call(
        finish_kernel,
        grid=(rows // block,),
        in_specs=specs,
        out_specs=pl.BlockSpec((block, width), mine),
        out_shape=jax.ShapeDtypeStruct(w_query.shape, BF),
        input_output_aliases=aliases,
        name="finish",
    )(*operands)


def attention_kernel(
    in_scale, block, size, rank_ref, y_q, y_k, y_v, cot, cos_ref, sin_ref,
    out, grad_q, grad_k, grad_v, keys, values, keys_t, values_t, sum_k, sum_v,
):
    length = y_k.shape[0]
    rows_each = length // size
    count = length // block
    per = block // rows_each
    head_scale = HD ** (-0.5)
    rank = rank_ref[0]

    def slot_rows(natural):
        mask = rank ^ natural
        slot = mask // 2 + mask % 2 * (size // 2)
        return pl.ds(pl.multiple_of(slot * rows_each, rows_each), rows_each)

    def table(ref, i):
        return jnp.concatenate([ref[slot_rows(i * per + j), :] for j in range(per)], axis=0)

    @pl.when(pl.program_id(0) == 0)
    def _():
        for i in range(count):
            rows = pl.ds(i * block, block)
            key = turned(table(y_k, i) * in_scale, table(cos_ref, i), table(sin_ref, i)).astype(BF)
            value = (table(y_v, i) * in_scale).astype(BF)
            keys[rows, :] = key
            values[rows, :] = value
            keys_t[:, rows] = key.T
            values_t[:, rows] = value.T
        sum_k[...] = jnp.zeros_like(sum_k)
        sum_v[...] = jnp.zeros_like(sum_v)

    for i in range(count):
        rows = pl.ds(i * block, block)
        cos = table(cos_ref, i)
        sin = table(sin_ref, i)
        query = turned(table(y_q, i) * in_scale, cos, sin).astype(BF)
        grad = cot[rows, :]
        spans = [pl.ds(0, i * block)] if i else []
        spans.append(rows)
        scores = []
        for span in spans:
            scores.append(nt(keys[span, :], query))
        t = lax.broadcasted_iota(jnp.int32, (block, block), 0)
        s = lax.broadcasted_iota(jnp.int32, (block, block), 1)
        scores[-1] = jnp.where(t <= s, scores[-1], -1e30)
        top = functools.reduce(
            jnp.maximum, [jnp.max(score, axis=0, keepdims=True) for score in scores]
        )
        powers = [jnp.exp((score - top) * head_scale) for score in scores]
        total = sum(jnp.sum(power, axis=0, keepdims=True) for power in powers)
        inverse = 1.0 / total
        probs = [power * inverse for power in powers]
        raws = [nt(values[span, :], grad) for span in spans]
        inner = sum(
            jnp.sum(prob * raw, axis=0, keepdims=True) for prob, raw in zip(probs, raws)
        )
        out_t = None
        query_t = None
        for span, prob, raw in zip(spans, probs, raws):
            low = prob.astype(BF)
            grad_low = (prob * (raw - inner) * head_scale).astype(BF)
            o_part = nn(values_t[:, span], low)
            q_part = nn(keys_t[:, span], grad_low)
            out_t = o_part if out_t is None else out_t + o_part
            query_t = q_part if query_t is None else query_t + q_part
            sum_v[span, :] += nn(low, grad)
            sum_k[span, :] += nn(grad_low, query)
        out[rows, :] = out_t.T.astype(BF)
        turned_q = turned(query_t.T, cos, -sin).astype(BF)
        for j in range(per):
            grad_q[slot_rows(i * per + j), :] = turned_q[j * rows_each : (j + 1) * rows_each]

    @pl.when(pl.program_id(0) == pl.num_programs(0) - 1)
    def _():
        for natural in range(size):
            rows = pl.ds(natural * rows_each, rows_each)
            grad_k[slot_rows(natural), :] = sum_k[rows, :]
            grad_v[slot_rows(natural), :] = sum_v[rows, :]


def attention(rank, size, projected, cotangent, cos, sin, in_scale, first, heads, key_at):
    length = projected.shape[0]
    rows_each = length // size
    block = rows_each * max(1, 256 // rows_each)
    whole = lambda h, r: (0, 0)
    head = lambda h, r: (0, h + first)
    mine = lambda h, r: (0, h)
    return pl.pallas_call(
        functools.partial(attention_kernel, in_scale, block, size),
        grid_spec=pltpu.PrefetchScalarGridSpec(
            num_scalar_prefetch=1,
            grid=(heads,),
            in_specs=[
                pl.BlockSpec((length, HD), head),
                pl.BlockSpec((length, HD), lambda h, r: (0, key_at)),
                pl.BlockSpec((length, HD), lambda h, r: (0, key_at + 1)),
                pl.BlockSpec((length, HD), head),
                pl.BlockSpec((length, HD), whole),
                pl.BlockSpec((length, HD), whole),
            ],
            out_specs=[
                pl.BlockSpec((length, HD), mine),
                pl.BlockSpec((length, HD), mine),
                pl.BlockSpec((length, HD), whole),
                pl.BlockSpec((length, HD), whole),
            ],
            scratch_shapes=[
                pltpu.VMEM((length, HD), BF),
                pltpu.VMEM((length, HD), BF),
                pltpu.VMEM((HD, length), BF),
                pltpu.VMEM((HD, length), BF),
                pltpu.VMEM((length, HD), F32),
                pltpu.VMEM((length, HD), F32),
            ],
        ),
        out_shape=[
            jax.ShapeDtypeStruct((length, heads * HD), BF),
            jax.ShapeDtypeStruct((length, heads * HD), BF),
            jax.ShapeDtypeStruct((length, HD), F32),
            jax.ShapeDtypeStruct((length, HD), F32),
        ],
        cost_estimate=pl.CostEstimate(
            flops=12 * heads * length * length * HD // 2,
            transcendentals=heads * length * length // 2,
            bytes_accessed=heads * length * HD * 10,
        ),
        name="attend",
    )(rank.reshape(1), projected, projected, projected, cotangent, cos, sin)


def per_device(
    tokens, cotangent, gain, w_query, w_key, w_value, moment_query, moment_key, moment_value
):
    rank = lax.axis_index("tensor")
    query_width = w_query.shape[1]
    key_width = w_key.shape[1]
    heads = query_width // HD
    width = tokens.shape[2]
    rows_each = tokens.shape[1]
    in_scale = width ** (-0.5)
    size = lax.axis_size("tensor")
    span = size // KVH
    levels = span.bit_length() - 1
    groups = 2 if heads % 2 == 0 else 1
    per_group = heads // groups
    group_width = per_group * HD

    inputs = tokens[0].astype(F32)
    reciprocal = lax.rsqrt(jnp.mean(inputs * inputs, axis=1, keepdims=True) + norm_eps)
    normed = (inputs * reciprocal * gain).astype(BF)
    stages = gather_blocks(normed, "tensor")
    cos, sin = rope_tables(rank, size, rows_each)

    own_pair = jnp.concatenate([w_key.T, w_value.T], axis=0)
    paired = own_pair.reshape(2, key_width, width)
    for level in range(levels):
        other = swap(paired, "tensor", 1 << level)
        higher = rank // 2**level % 2 == 1
        paired = jnp.where(
            higher,
            jnp.concatenate([other, paired], axis=1),
            jnp.concatenate([paired, other], axis=1),
        )
    w_turned = jnp.concatenate([w_query.T, own_pair], axis=0)
    w_pair, w_turned = lax.optimization_barrier((paired.reshape(2 * HD, width), w_turned))

    moment_pair = jnp.concatenate([moment_key.T, moment_value.T], axis=0)
    shrink = learn_rate * keep_rate
    held_back = line_gather(
        jnp.concatenate(
            [(shrink * moment_query).astype(BF), (shrink * moment_pair).astype(BF).T], axis=1
        ),
        "dp",
    )

    done = None
    for first, even, odd in stages:
        done = project(first, even, odd, rows_each, size, w_query, w_pair, done)
    projected = done[0].reshape(size * rows_each, -1)
    normed_all = done[1].reshape(size * rows_each, width)

    def weight_terms(grad):
        return (
            jnp.einsum("sd,sc->dc", normed_all, grad, preferred_element_type=F32) * in_scale
        ).astype(BF)

    outs = []
    grads = []
    terms = []
    key_local = 0.0
    value_local = 0.0
    for g in range(groups):
        if terms:
            projected = after(projected, terms[-1])
        out, grad_q, grad_k, grad_v = attention(
            rank, size, projected, cotangent[0], cos, sin, in_scale,
            g * per_group, per_group, heads,
        )
        outs.append(out)
        grads.append(grad_q)
        key_local = key_local + grad_k
        value_local = value_local + grad_v
        if g < groups - 1:
            terms.append(weight_terms(grad_q))

    current = jnp.stack([key_local, value_local]).astype(BF).astype(F32)
    masks = slot_masks(size)
    for level in reversed(range(levels)):
        middle = current.shape[2] // 2
        higher = rank // 2**level % 2 == 1
        outgoing = jnp.where(higher, current[:, :, :middle], current[:, :, middle:])
        retained = jnp.where(higher, current[:, :, middle:], current[:, :, :middle])
        arrived = swap(outgoing.astype(BF), "tensor", 1 << level)
        places = [slot_of(mask ^ 1 << level, size) * rows_each for mask in masks]
        arrived = jnp.concatenate([arrived[:, at : at + rows_each] for at in places], axis=1)
        current = retained + arrived.astype(F32)
    first = (rank % span) * key_width
    cos_own = lax.dynamic_slice_in_dim(cos, first, key_width, 1)
    sin_own = lax.dynamic_slice_in_dim(sin, first, key_width, 1)
    even = jnp.arange(key_width) % 2 == 0
    partner = jnp.where(
        even[None, :], jnp.roll(current[0], -1, axis=1), jnp.roll(current[0], 1, axis=1)
    )
    grad_key = (current[0] * cos_own - partner * sin_own).astype(BF)
    grad_pair = jnp.concatenate([grad_key, current[1].astype(BF)], axis=1)
    terms.append(weight_terms(jnp.concatenate([grads[-1], grad_pair], axis=1)))
    grad_all = after(jnp.concatenate(grads + [grad_pair], axis=1), terms[-1])
    half = size * rows_each // 2

    def rows_grad(part):
        return (jnp.dot(part, w_turned, preferred_element_type=F32) * in_scale).astype(BF)

    odd = rows_grad(grad_all[half:])
    even = rows_grad(after(grad_all[:half], odd))
    grad_normed = scatter_blocks(even, odd, "tensor")
    unit_rows = inputs * reciprocal
    grad_unit = grad_normed * gain
    inner = jnp.mean(grad_unit * unit_rows, axis=1, keepdims=True)
    grad_tokens = (reciprocal * (grad_unit - unit_rows * inner)).astype(BF)[None]

    sums = [line_scatter(term, "dp") for term in terms]
    fulls = [line_gather(part.astype(BF), "dp") for part in sums]
    square = sum(jnp.sum(part * part) for part in sums)
    total = sum_everywhere(square.reshape(1, 1))
    count_all = 1.0 * D * HD * (HEADS + 2 * KVH)
    factor = lax.rsqrt(total / count_all + stat_eps)

    moment_query, moment_key, moment_value = lax.optimization_barrier(
        (moment_query, moment_key, moment_value, square)
    )[:3]
    moment_pair = jnp.concatenate([moment_key.T, moment_value.T], axis=0)
    next_query = keep_rate * moment_query + factor * jnp.concatenate(
        sums[:-1] + [sums[-1][:, :group_width]], axis=1
    )
    next_pair = keep_rate * moment_pair + factor * sums[-1][:, group_width:].T
    fresh_query = None
    for g, full in enumerate(fulls):
        fresh_query = finish_query(
            factor.reshape(1, 1), w_query, held_back, full, g, group_width, fresh_query
        )
    full_pair = fulls[-1][:, group_width:].T.astype(F32)
    fresh_pair = (
        own_pair.astype(F32)
        - held_back[:, query_width:].T.astype(F32)
        - learn_rate * factor * full_pair
    ).astype(BF)
    return (
        jnp.concatenate(outs, axis=1)[None],
        grad_tokens,
        fresh_query,
        fresh_pair[:key_width].T,
        fresh_pair[key_width:].T,
        next_query,
        next_pair[:key_width].T,
        next_pair[key_width:].T,
    )


def solution(mesh):
    placed = (
        P("dp", "tensor", None),
        P("dp", None, "tensor"),
        P(),
        P(None, "tensor"),
        P(None, "tensor"),
        P(None, "tensor"),
        P("dp", "tensor"),
        P("dp", "tensor"),
        P("dp", "tensor"),
    )
    return jax.shard_map(
        per_device,
        mesh=mesh,
        in_specs=placed,
        out_specs=(
            P("dp", None, "tensor"),
            P("dp", "tensor", None),
            P(None, "tensor"),
            P(None, "tensor"),
            P(None, "tensor"),
            P("dp", "tensor"),
            P("dp", "tensor"),
            P("dp", "tensor"),
        ),
        check_vma=False,
    )
```

```python
import functools

import jax
import jax.numpy as jnp
from jax import lax
from jax.experimental import pallas as pl
from jax.experimental.pallas import tpu as pltpu
from jax.sharding import PartitionSpec as P


D = 4096
HEADS = 32
KVH = 4
HD = 128

rope_base = 1000000.0
norm_eps = 1e-06
stat_eps = 1e-06
learn_rate = 0.05
keep_rate = 0.9

BF = jnp.bfloat16
F32 = jnp.float32


def swap(shard, axis, mask):
    return lax.ppermute(shard, axis, [(i, i ^ mask) for i in range(lax.axis_size(axis))])


def after(value, *others):
    return lax.optimization_barrier((value,) + others)[0]


def slot_masks(size):
    return list(range(0, size, 2)) + list(range(1, size, 2))


def slot_of(mask, size):
    return mask // 2 + mask % 2 * (size // 2)


def gather_blocks(block, axis):
    size = lax.axis_size(axis)
    if size == 8:
        cut = block.shape[0] // 2
        top, low = block[:cut], block[cut:]
        y_top = swap(top, axis, 4)
        x_low = swap(low, axis, 2)
        y_low = swap(low, axis, 4)
        x_top = swap(top, axis, 2)
        far_top = swap(y_top, axis, 2)
        far_low = swap(x_low, axis, 4)
        even = {"t": top, "l": low, "xt": x_top, "xl": x_low, "yt": y_top, "yl": y_low}
        odd = [swap(piece, axis, 1) for piece in even.values()]
        far = [swap(far_top, axis, 1), swap(far_low, axis, 1)]
        return [(0, list(even.values()), odd), (3, [far_top, far_low], far)]
    even = [block]
    for level in range(1, size.bit_length() - 1):
        even = even + [swap(piece, axis, 1 << level) for piece in even]
    return [(0, even, [swap(piece, axis, 1) for piece in even])]


def scatter_blocks(even, odd, axis):
    size = lax.axis_size(axis)
    folded = (even.astype(F32) + swap(odd, axis, 1).astype(F32)).astype(BF)
    folded = folded.reshape(size // 2, -1, even.shape[1])
    if size == 8:
        cut = folded.shape[1] // 2
        top = swap(jnp.concatenate([folded[1, :cut], folded[3, :cut]], axis=0), axis, 2)
        bottom = swap(jnp.concatenate([folded[2, cut:], folded[3, cut:]], axis=0), axis, 4)
        top_y = (folded[2, :cut].astype(F32) + top[cut:].astype(F32)).astype(BF)
        bottom_x = (folded[1, cut:].astype(F32) + bottom[cut:].astype(F32)).astype(BF)
        top_y = swap(top_y, axis, 4)
        bottom_x = swap(bottom_x, axis, 2)
        own = folded[0].astype(F32)
        first = own[:cut] + top[:cut].astype(F32) + top_y.astype(F32)
        second = own[cut:] + bottom[:cut].astype(F32) + bottom_x.astype(F32)
        return jnp.concatenate([first, second], axis=0)
    held = {mask: folded[mask // 2].astype(F32) for mask in range(0, size, 2)}
    for level in range(1, size.bit_length() - 1):
        bit = 1 << level
        for mask in sorted(mask for mask in held if mask & bit):
            piece = held.pop(mask)
            held[mask ^ bit] = held[mask ^ bit] + swap(piece.astype(BF), axis, bit).astype(F32)
    return held[0]


def line_pairs(size, step, right):
    if right:
        return [(z, z + 1) for z in range(min(step, size - 1))]
    return [(z, z - 1) for z in range(max(size - step, 1), size)]


def line_scatter(terms, axis):
    size = lax.axis_size(axis)
    z = lax.axis_index(axis)
    rows = terms.shape[0] // size

    def own(index):
        return lax.dynamic_slice_in_dim(terms, index * rows, rows, 0)

    from_left = None
    from_right = None
    for step in range(1, size):
        if from_left is not None:
            terms, from_left, from_right = lax.optimization_barrier(
                (terms, from_left, from_right)
            )
        right = own((z + size - step) % size)
        left = own((z + step) % size)
        if from_left is not None:
            right = (right.astype(F32) + from_left.astype(F32)).astype(BF)
            left = (left.astype(F32) + from_right.astype(F32)).astype(BF)
        from_left = lax.ppermute(right, axis, line_pairs(size, step, True))
        from_right = lax.ppermute(left, axis, line_pairs(size, step, False))
    if size > 1:
        terms, from_left, from_right = lax.optimization_barrier((terms, from_left, from_right))
        return own(z).astype(F32) + from_left.astype(F32) + from_right.astype(F32)
    return own(z).astype(F32)


def line_gather(shard, axis):
    size = lax.axis_size(axis)
    rights = [shard]
    lefts = [shard]
    for step in range(1, size):
        pairs = [(i, i + 1) for i in range(step - 1, size - 1)]
        rights.append(lax.ppermute(rights[-1], axis, pairs))
        pairs = [(i, i - 1) for i in range(1, size - step + 1)]
        lefts.append(lax.ppermute(lefts[-1], axis, pairs))
    return [shard] + rights[1:] + lefts[1:]


def sum_everywhere(value):
    for axis in ("tensor", "dp"):
        for level in range(lax.axis_size(axis).bit_length() - 1):
            value = value + swap(value, axis, 1 << level)
    return value[0, 0]


def rope_tables(rank, size, rows):
    blocks = rank ^ jnp.array(slot_masks(size), jnp.int32)
    places = (blocks[:, None] * rows + jnp.arange(rows, dtype=jnp.int32)[None, :]).reshape(-1)
    within = jnp.arange(HD, dtype=jnp.int32) // 2
    rates = jnp.power(F32(rope_base), within.astype(F32) * (-2.0 / HD))
    angle = places.astype(F32)[:, None] * rates[None, :]
    even = jnp.arange(HD, dtype=jnp.int32) % 2 == 0
    sin = jnp.sin(angle)
    return jnp.cos(angle), jnp.where(even[None, :], -sin, sin)


def turned(matrix, cos, sin):
    lane = lax.broadcasted_iota(jnp.int32, matrix.shape, 1)
    partner = jnp.where(
        lane % 2 == 0, pltpu.roll(matrix, HD - 1, 1), pltpu.roll(matrix, 1, 1)
    )
    return matrix * cos + partner * sin


def nt(a, b):
    return lax.dot_general(a, b, (((1,), (1,)), ((), ())), preferred_element_type=F32)


def nn(a, b):
    return lax.dot_general(a, b, (((1,), (0,)), ((), ())), preferred_element_type=F32)


def project_kernel(counts, *refs):
    even = refs[: counts[0]]
    odd = refs[counts[0] : counts[0] + counts[1]]
    w_query, w_pair = refs[counts[0] + counts[1] :][:2]
    out, rows_out = refs[-2:]
    query_width = w_query.shape[1]
    step = pl.program_id(0)

    @pl.when(step == 0)
    def _():
        out[...] = jnp.zeros_like(out)

    rows = jnp.concatenate([piece[...] for piece in even + odd], axis=0)
    rows_out[...] = rows.reshape(rows_out.shape)
    query = nn(rows, w_query[...])
    pair = nt(rows, w_pair[...])
    out[:, :, :query_width] += query.reshape(2, -1, query_width)
    out[:, :, query_width:] += pair.reshape(2, -1, w_pair.shape[0])


def project(first, even, odd, rows_each, size, w_query, w_pair, previous):
    width = w_query.shape[0]
    columns = w_query.shape[1] + w_pair.shape[0]
    half = size // 2 * rows_each
    rows = sum(piece.shape[0] for piece in even)
    chunk = min(width, 1024)
    pieces = list(even) + list(odd)
    operands = pieces + [w_query, w_pair]
    specs = [pl.BlockSpec((piece.shape[0], chunk), lambda k: (0, k)) for piece in pieces]
    specs.append(pl.BlockSpec((chunk, w_query.shape[1]), lambda k: (k, 0)))
    specs.append(pl.BlockSpec((w_pair.shape[0], chunk), lambda k: (0, k)))
    aliases = {}
    if previous is not None:
        aliases = {len(operands): 0, len(operands) + 1: 1}
        operands = operands + list(previous)
        specs = specs + [pl.BlockSpec(memory_space=pl.ANY)] * 2
    at = first * rows_each // rows
    return pl.pallas_call(
        functools.partial(project_kernel, (len(even), len(odd))),
        grid=(width // chunk,),
        in_specs=specs,
        out_specs=[
            pl.BlockSpec((2, rows, columns), lambda k: (0, at, 0)),
            pl.BlockSpec((2, rows, chunk), lambda k: (0, at, k)),
        ],
        out_shape=[
            jax.ShapeDtypeStruct((2, half, columns), F32),
            jax.ShapeDtypeStruct((2, half, width), BF),
        ],
        input_output_aliases=aliases,
        cost_estimate=pl.CostEstimate(
            flops=4 * rows * width * columns,
            transcendentals=0,
            bytes_accessed=8 * rows * width + 2 * width * columns,
        ),
        name="project",
    )(*operands)


def finish_kernel(size, at, width, paired, place_ref, factor_ref, w_ref, *refs):
    count = 2 * size - 1
    pair_ref = refs[0] if paired else None
    refs = refs[1:] if paired else refs
    held_refs, sum_refs = refs[:count], refs[count : 2 * count]
    outs = refs[2 * count + (at > 0) : -4]
    held, total, held_sem, total_sem = refs[-4:]
    z = place_ref[0]
    rows, columns = sum_refs[0].shape
    scaled = learn_rate * factor_ref[0, 0]

    def copies(block):
        found = []
        for distance in range(-(size - 1), size):
            if distance <= 0:
                which = -distance if distance else 0
            else:
                which = size - 1 + distance
            here = pl.ds(block * rows, rows)
            found.append(
                (
                    distance,
                    pltpu.make_async_copy(
                        held_refs[which].at[:, pl.ds(at, columns)], held.at[here], held_sem.at[block]
                    ),
                    pltpu.make_async_copy(
                        sum_refs[which], total.at[here], total_sem.at[block]
                    ),
                )
            )
        return found

    step = pl.program_id(0)

    @pl.when(step == 0)
    def _():
        for block in range(size):
            for distance, one, two in copies(block):

                @pl.when(z + distance == block)
                def _():
                    one.start()
                    two.start()

    for block in range(size):

        @pl.when(step == block)
        def _():
            _, one, two = copies(block)[0]
            one.wait()
            two.wait()
            here = pl.ds(block * rows, rows)
            change = held[here, :].astype(F32) + scaled * total[here, :].astype(F32)
            outs[0][...] = (w_ref[...].astype(F32) - change[:, :width]).astype(BF)
            if paired:
                fresh = (pair_ref[...].astype(F32) - change[:, width:].T).astype(BF)
                middle = fresh.shape[0] // 2
                outs[1][...] = fresh[:middle]
                outs[2][...] = fresh[middle:]


def finish(z, factor, w_query, own_pair, held_pieces, sum_pieces, group, width, previous):
    size = (len(sum_pieces) + 1) // 2
    rows, columns = sum_pieces[0].shape
    paired = columns > width
    mine = lambda r, z: (r, group)
    operands = [z.reshape(1), factor.reshape(1, 1), w_query]
    specs = [pl.BlockSpec(memory_space=pltpu.SMEM), pl.BlockSpec((rows, width), mine)]
    out_specs = [pl.BlockSpec((rows, width), mine)]
    out_shape = [jax.ShapeDtypeStruct(w_query.shape, BF)]
    if paired:
        pair_rows = own_pair.shape[0]
        operands.append(own_pair)
        specs.append(pl.BlockSpec((pair_rows, rows), lambda r, z: (0, r)))
        for _ in range(2):
            out_specs.append(pl.BlockSpec((pair_rows // 2, rows), lambda r, z: (0, r)))
            out_shape.append(jax.ShapeDtypeStruct((pair_rows // 2, own_pair.shape[1]), BF))
    operands += list(held_pieces) + list(sum_pieces)
    specs += [pl.BlockSpec(memory_space=pl.ANY)] * (2 * len(sum_pieces))
    aliases = {}
    if previous is not None:
        aliases = {len(operands): 0}
        operands.append(previous)
        specs.append(pl.BlockSpec(memory_space=pl.ANY))
    return pl.pallas_call(
        functools.partial(finish_kernel, size, group * width, width, paired),
        grid_spec=pltpu.PrefetchScalarGridSpec(
            num_scalar_prefetch=1,
            grid=(size,),
            in_specs=specs,
            out_specs=out_specs,
            scratch_shapes=[
                pltpu.VMEM((size * rows, columns), BF),
                pltpu.VMEM((size * rows, columns), BF),
                pltpu.SemaphoreType.DMA((size,)),
                pltpu.SemaphoreType.DMA((size,)),
            ],
        ),
        out_shape=out_shape,
        input_output_aliases=aliases,
        name="finish",
    )(*operands)


def attention_kernel(
    in_scale, block, size, rank_ref, y_q, y_k, y_v, cot, cos_ref, sin_ref,
    out, grad_q, grad_k, grad_v, keys, values, keys_t, values_t, sum_k, sum_v,
):
    length = y_k.shape[0]
    rows_each = length // size
    count = length // block
    per = block // rows_each
    head_scale = HD ** (-0.5)
    rank = rank_ref[0]

    def slot_rows(natural):
        mask = rank ^ natural
        slot = mask // 2 + mask % 2 * (size // 2)
        return pl.ds(pl.multiple_of(slot * rows_each, rows_each), rows_each)

    def table(ref, i):
        return jnp.concatenate([ref[slot_rows(i * per + j), :] for j in range(per)], axis=0)

    @pl.when(pl.program_id(0) == 0)
    def _():
        for i in range(count):
            rows = pl.ds(i * block, block)
            key = turned(table(y_k, i) * in_scale, table(cos_ref, i), table(sin_ref, i)).astype(BF)
            value = (table(y_v, i) * in_scale).astype(BF)
            keys[rows, :] = key
            values[rows, :] = value
            keys_t[:, rows] = key.T
            values_t[:, rows] = value.T
        sum_k[...] = jnp.zeros_like(sum_k)
        sum_v[...] = jnp.zeros_like(sum_v)

    for i in range(count):
        rows = pl.ds(i * block, block)
        cos = table(cos_ref, i)
        sin = table(sin_ref, i)
        query = turned(table(y_q, i) * in_scale, cos, sin).astype(BF)
        grad = cot[rows, :]
        spans = [pl.ds(0, i * block)] if i else []
        spans.append(rows)
        scores = []
        for span in spans:
            scores.append(nt(keys[span, :], query))
        t = lax.broadcasted_iota(jnp.int32, (block, block), 0)
        s = lax.broadcasted_iota(jnp.int32, (block, block), 1)
        scores[-1] = jnp.where(t <= s, scores[-1], -1e30)
        top = functools.reduce(
            jnp.maximum, [jnp.max(score, axis=0, keepdims=True) for score in scores]
        )
        powers = [jnp.exp((score - top) * head_scale) for score in scores]
        total = sum(jnp.sum(power, axis=0, keepdims=True) for power in powers)
        inverse = 1.0 / total
        probs = [power * inverse for power in powers]
        raws = [nt(values[span, :], grad) for span in spans]
        inner = sum(
            jnp.sum(prob * raw, axis=0, keepdims=True) for prob, raw in zip(probs, raws)
        )
        out_t = None
        query_t = None
        for span, prob, raw in zip(spans, probs, raws):
            low = prob.astype(BF)
            grad_low = (prob * (raw - inner) * head_scale).astype(BF)
            o_part = nn(values_t[:, span], low)
            q_part = nn(keys_t[:, span], grad_low)
            out_t = o_part if out_t is None else out_t + o_part
            query_t = q_part if query_t is None else query_t + q_part
            sum_v[span, :] += nn(low, grad)
            sum_k[span, :] += nn(grad_low, query)
        out[rows, :] = out_t.T.astype(BF)
        turned_q = turned(query_t.T, cos, -sin).astype(BF)
        for j in range(per):
            grad_q[slot_rows(i * per + j), :] = turned_q[j * rows_each : (j + 1) * rows_each]

    @pl.when(pl.program_id(0) == pl.num_programs(0) - 1)
    def _():
        for natural in range(size):
            rows = pl.ds(natural * rows_each, rows_each)
            grad_k[slot_rows(natural), :] = sum_k[rows, :]
            grad_v[slot_rows(natural), :] = sum_v[rows, :]


def attention(rank, size, projected, cotangent, cos, sin, in_scale, first, heads, key_at):
    length = projected.shape[0]
    rows_each = length // size
    block = rows_each * max(1, 256 // rows_each)
    whole = lambda h, r: (0, 0)
    head = lambda h, r: (0, h + first)
    mine = lambda h, r: (0, h)
    return pl.pallas_call(
        functools.partial(attention_kernel, in_scale, block, size),
        grid_spec=pltpu.PrefetchScalarGridSpec(
            num_scalar_prefetch=1,
            grid=(heads,),
            in_specs=[
                pl.BlockSpec((length, HD), head),
                pl.BlockSpec((length, HD), lambda h, r: (0, key_at)),
                pl.BlockSpec((length, HD), lambda h, r: (0, key_at + 1)),
                pl.BlockSpec((length, HD), head),
                pl.BlockSpec((length, HD), whole),
                pl.BlockSpec((length, HD), whole),
            ],
            out_specs=[
                pl.BlockSpec((length, HD), mine),
                pl.BlockSpec((length, HD), mine),
                pl.BlockSpec((length, HD), whole),
                pl.BlockSpec((length, HD), whole),
            ],
            scratch_shapes=[
                pltpu.VMEM((length, HD), BF),
                pltpu.VMEM((length, HD), BF),
                pltpu.VMEM((HD, length), BF),
                pltpu.VMEM((HD, length), BF),
                pltpu.VMEM((length, HD), F32),
                pltpu.VMEM((length, HD), F32),
            ],
        ),
        out_shape=[
            jax.ShapeDtypeStruct((length, heads * HD), BF),
            jax.ShapeDtypeStruct((length, heads * HD), BF),
            jax.ShapeDtypeStruct((length, HD), F32),
            jax.ShapeDtypeStruct((length, HD), F32),
        ],
        cost_estimate=pl.CostEstimate(
            flops=12 * heads * length * length * HD // 2,
            transcendentals=heads * length * length // 2,
            bytes_accessed=heads * length * HD * 10,
        ),
        name="attend",
    )(rank.reshape(1), projected, projected, projected, cotangent, cos, sin)


def per_device(
    tokens, cotangent, gain, w_query, w_key, w_value, moment_query, moment_key, moment_value
):
    rank = lax.axis_index("tensor")
    query_width = w_query.shape[1]
    key_width = w_key.shape[1]
    heads = query_width // HD
    width = tokens.shape[2]
    rows_each = tokens.shape[1]
    in_scale = width ** (-0.5)
    size = lax.axis_size("tensor")
    span = size // KVH
    levels = span.bit_length() - 1
    groups = 2 if heads % 2 == 0 else 1
    per_group = heads // groups
    group_width = per_group * HD

    inputs = tokens[0].astype(F32)
    reciprocal = lax.rsqrt(jnp.mean(inputs * inputs, axis=1, keepdims=True) + norm_eps)
    normed = (inputs * reciprocal * gain).astype(BF)
    stages = gather_blocks(normed, "tensor")
    cos, sin = rope_tables(rank, size, rows_each)

    own_pair = jnp.concatenate([w_key.T, w_value.T], axis=0)
    paired = own_pair.reshape(2, key_width, width)
    for level in range(levels):
        other = swap(paired, "tensor", 1 << level)
        higher = rank // 2**level % 2 == 1
        paired = jnp.where(
            higher,
            jnp.concatenate([other, paired], axis=1),
            jnp.concatenate([paired, other], axis=1),
        )
    w_turned = jnp.concatenate([w_query.T, own_pair], axis=0)
    w_pair, w_turned = lax.optimization_barrier((paired.reshape(2 * HD, width), w_turned))

    moment_pair = jnp.concatenate([moment_key.T, moment_value.T], axis=0)
    shrink = learn_rate * keep_rate
    held_back = line_gather(
        jnp.concatenate(
            [(shrink * moment_query).astype(BF), (shrink * moment_pair).astype(BF).T], axis=1
        ),
        "dp",
    )

    done = None
    for first, even, odd in stages:
        done = project(first, even, odd, rows_each, size, w_query, w_pair, done)
    projected = done[0].reshape(size * rows_each, -1)
    normed_all = done[1].reshape(size * rows_each, width)

    def weight_terms(grad):
        return (
            jnp.einsum("sd,sc->dc", normed_all, grad, preferred_element_type=F32) * in_scale
        ).astype(BF)

    outs = []
    grads = []
    terms = []
    key_local = 0.0
    value_local = 0.0
    for g in range(groups):
        if terms:
            projected = after(projected, terms[-1])
        out, grad_q, grad_k, grad_v = attention(
            rank, size, projected, cotangent[0], cos, sin, in_scale,
            g * per_group, per_group, heads,
        )
        outs.append(out)
        grads.append(grad_q)
        key_local = key_local + grad_k
        value_local = value_local + grad_v
        if g < groups - 1:
            terms.append(weight_terms(grad_q))

    current = jnp.stack([key_local, value_local]).astype(BF).astype(F32)
    masks = slot_masks(size)
    for level in reversed(range(levels)):
        middle = current.shape[2] // 2
        higher = rank // 2**level % 2 == 1
        outgoing = jnp.where(higher, current[:, :, :middle], current[:, :, middle:])
        retained = jnp.where(higher, current[:, :, middle:], current[:, :, :middle])
        arrived = swap(outgoing.astype(BF), "tensor", 1 << level)
        places = [slot_of(mask ^ 1 << level, size) * rows_each for mask in masks]
        arrived = jnp.concatenate([arrived[:, at : at + rows_each] for at in places], axis=1)
        current = retained + arrived.astype(F32)
    first = (rank % span) * key_width
    cos_own = lax.dynamic_slice_in_dim(cos, first, key_width, 1)
    sin_own = lax.dynamic_slice_in_dim(sin, first, key_width, 1)
    even = jnp.arange(key_width) % 2 == 0
    partner = jnp.where(
        even[None, :], jnp.roll(current[0], -1, axis=1), jnp.roll(current[0], 1, axis=1)
    )
    grad_key = (current[0] * cos_own - partner * sin_own).astype(BF)
    grad_pair = jnp.concatenate([grad_key, current[1].astype(BF)], axis=1)
    terms.append(weight_terms(jnp.concatenate([grads[-1], grad_pair], axis=1)))
    grad_all = after(jnp.concatenate(grads + [grad_pair], axis=1), terms[-1])
    half = size * rows_each // 2

    def rows_grad(part):
        return (jnp.dot(part, w_turned, preferred_element_type=F32) * in_scale).astype(BF)

    odd = rows_grad(grad_all[half:])
    even = rows_grad(after(grad_all[:half], odd))
    grad_normed = scatter_blocks(even, odd, "tensor")
    unit_rows = inputs * reciprocal
    grad_unit = grad_normed * gain
    inner = jnp.mean(grad_unit * unit_rows, axis=1, keepdims=True)
    grad_tokens = (reciprocal * (grad_unit - unit_rows * inner)).astype(BF)[None]

    sums = [line_scatter(term, "dp") for term in terms]
    fulls = [line_gather(part.astype(BF), "dp") for part in sums]
    square = sum(jnp.sum(part * part) for part in sums)
    total = sum_everywhere(square.reshape(1, 1))
    count_all = 1.0 * D * HD * (HEADS + 2 * KVH)
    factor = lax.rsqrt(total / count_all + stat_eps)

    moment_query, moment_pair = lax.optimization_barrier((moment_query, moment_pair, square))[:2]
    next_query = keep_rate * moment_query + factor * jnp.concatenate(
        sums[:-1] + [sums[-1][:, :group_width]], axis=1
    )
    next_pair = keep_rate * moment_pair + factor * sums[-1][:, group_width:].T
    fresh = [None]
    for g, full in enumerate(fulls):
        fresh = finish(
            lax.axis_index("dp"), factor, w_query, own_pair, held_back, full, g, group_width,
            fresh[0],
        )
    return (
        jnp.concatenate(outs, axis=1)[None],
        grad_tokens,
        fresh[0],
        fresh[1].T,
        fresh[2].T,
        next_query,
        next_pair[:key_width].T,
        next_pair[key_width:].T,
    )


def solution(mesh):
    placed = (
        P("dp", "tensor", None),
        P("dp", None, "tensor"),
        P(),
        P(None, "tensor"),
        P(None, "tensor"),
        P(None, "tensor"),
        P("dp", "tensor"),
        P("dp", "tensor"),
        P("dp", "tensor"),
    )
    return jax.shard_map(
        per_device,
        mesh=mesh,
        in_specs=placed,
        out_specs=(
            P("dp", None, "tensor"),
            P("dp", "tensor", None),
            P(None, "tensor"),
            P(None, "tensor"),
            P(None, "tensor"),
            P("dp", "tensor"),
            P("dp", "tensor"),
            P("dp", "tensor"),
        ),
        check_vma=False,
    )
```
